128 devices in a mesh: row: 8 (over y, x_hi), col: 16 (over z, x_lo, core).
Axes of the slice: x: 4 (x_hi: 2, x_lo: 2; x = x_hi * 2 + x_lo), y: 4, z: 4, core: 2. Of those that a mesh axis runs over, the one named last changes fastest.
Arguments:
- h_slab: bfloat16 [4096, 96000], P('row', 'col'), may hold values from -0.01953125 to 0.01953125
- vectors: bfloat16 [96000, 1024], P('col'), may hold values from -6 to 6
- left_rows: bfloat16 [4096, 1024], P('row'), may hold values from -0.09375 to 0.09375
Outputs:
- projected: float32 [1024, 1024], replicated
The draws below stay inside these ranges and needn't reach their ends.
All inputs are finite; a program needn't handle non-finite values.
Results may differ from the reference program's by a relative error of at most 0.0003.
Values sent between devices are 32-bit elements; how exact they have to be, the bound alone decides.
A program may use at most 128 MiB of HBM per device.

```python
import jax
import jax.numpy as jnp
from jax import lax

ORDER = 96000
NVEC = 1024
SLAB_ROWS = 4096


def block_levels(rng, dims, split, smallest, high):
    def one(position, parts):
        steps = jax.random.uniform(jax.random.fold_in(jax.random.fold_in(rng, 6), position), (parts,), jnp.float32, smallest / len(split), high / len(split))
        return jnp.repeat(jnp.exp(steps), dims[position] // parts).reshape((-1,) + (1,) * (len(dims) - position - 1))

    level = one(*split[0])
    for cut in split[1:]:
        level = level * one(*cut)
    return level


def bell_draw(stream_key, shape, deviation, most, shards=(), kind=jnp.bfloat16):
    result = jax.random.normal(stream_key, shape, jnp.float32) * deviation
    if len(shards) > 0:
        result = block_levels(stream_key, shape, shards, -0.22, 0.18) * result
    return jnp.clip(result, min=-most, max=most).astype(kind)


def setup_inputs(seed: int = 0) -> dict:
    splits = jax.random.split(jax.random.key(seed), 4)
    return {
        "h_slab": bell_draw(splits[0], (SLAB_ROWS, ORDER), ORDER ** -0.5, 0.01953125, ((0, 8), (1, 16))),
        "vectors": bell_draw(splits[1], (ORDER, NVEC), 1.0, 6.0, ((0, 16),)),
        "left_rows": bell_draw(splits[2], (SLAB_ROWS, NVEC), SLAB_ROWS ** -0.5, 0.09375, ((0, 8),)),
    }


def reference(h_slab, vectors, left_rows):
    product = jnp.dot(h_slab, vectors, preferred_element_type=jnp.float32)
    left_wide = left_rows.astype(jnp.float32)
    projected = jnp.dot(left_wide.T, product, precision=lax.Precision.HIGHEST)
    return projected
```

```python
import functools

import jax
import jax.numpy as jnp
from jax import lax
from jax.experimental import pallas as pl
from jax.experimental.pallas import tpu as pltpu
from jax.sharding import PartitionSpec as P

MESH = pl.DeviceIdType.MESH
F32 = jnp.float32
BF16 = jnp.bfloat16
DEPTH = 6000
ROWS = 512
HALF = 256
NVEC = 1024
CUTS = ((0, 2048), (2048, 4096), (4096, 6000))
A, A2 = 144, 72
B, B2 = 112, 56
ROTATIONS = ((0, 24), (24, 24), (48, 16))
NMSG = 160
CONTRACT0 = (((0,), (0,)), ((), ()))


def kernel(h_hbm, v_hbm, l_hbm, out, h, v, l, p, dr, zr1, zr2, xb, zb1, zb2, xa, pf, pfr, bhl, rp, rr, lsem, ssem, rsem):
    row, col = lax.axis_index("row"), lax.axis_index("col")
    y, xh = row // 2, row % 2
    z, xl, c = col // 4, (col // 2) % 2, col % 2
    x = xh * 2 + xl

    def dev(dx=0, dy=0, dz=0, core=None, px=None):
        nx = (x + dx) % 4 if px is None else px
        ny, nz = (y + dy) % 4, (z + dz) % 4
        nc = c if core is None else core
        return (ny * 2 + nx // 2, nz * 4 + (nx % 2) * 2 + nc)

    partner = dev(core=1 - c)
    mate = dev(px=xh * 2 + 1 - xl)

    zs = [(z + 2) % 4, (z + 1) % 4, (z + 3) % 4, z]
    lanes = [pl.ds(pl.multiple_of(q * 256, 256), 256) for q in zs]
    loads = []

    def load(src, dst):
        cp = pltpu.make_async_copy(src, dst, lsem.at[len(loads)])
        cp.start()
        loads.append(cp)
        return cp

    first = []
    for lo, hi in CUTS:
        k = pl.ds(lo, hi - lo)
        first.append((load(h_hbm.at[k, :], h.at[k, :]), load(v_hbm.at[k, lanes[0]], v.at[0, k, :])))
    rest = [load(v_hbm.at[:, lanes[s]], v.at[s]) for s in (1, 2, 3)]
    lload = load(l_hbm.at[:, pl.ds(pl.multiple_of(c * 512, 512), 512)], l)

    barrier = pltpu.get_barrier_semaphore()
    peers = [partner]
    for d in (1, 2, 3):
        peers += [dev(dx=d), dev(dy=d), dev(dz=d), dev(dx=2, dy=d)]
    for peer in peers:
        pl.semaphore_signal(barrier, inc=1, device_id=peer, device_id_type=MESH)

    sent = []

    def send(src, dst, device):
        i = len(sent)
        rc = pltpu.make_async_remote_copy(
            src_ref=src, dst_ref=dst, send_sem=ssem.at[i], recv_sem=rsem.at[i], device_id=device, device_id_type=MESH
        )
        rc.start()
        sent.append(rc)
        return rc

    def dot(s, lo, hi):
        k = pl.ds(lo, hi - lo)
        return lax.dot_general(h[k, :], v[s, k, :], CONTRACT0, preferred_element_type=F32).reshape(2, HALF, 256)

    def swap(s):
        return send(p.at[s, 1 - c], dr.at[s], partner)

    def settle(s, rc):
        rc.wait_recv()
        p[s, c] = p[s, c] + dr[s]

    ours = pl.ds(pl.multiple_of(xl * 128, 128), 128)
    theirs = pl.ds(pl.multiple_of(128 - xl * 128, 128), 128)

    def xb_send(s):
        return send(p.at[s, c, pl.ds(A, B), theirs], xb.at[s], mate)

    def xb_settle(s, rc):
        rc.wait_recv()
        p[s, c, pl.ds(A, B), ours] = p[s, c, pl.ds(A, B), ours] + xb[s]

    up, down = dev(dz=1), dev(dz=3)
    a_lo, a_hi = pl.ds(0, A2), pl.ds(A2, A2)
    b_lo, b_hi = pl.ds(A, B2), pl.ds(A + B2, B2)

    for i, (lo, hi) in enumerate(CUTS):
        first[i][0].wait()
        first[i][1].wait()
        if i == 0:
            p[0] = dot(0, lo, hi)
        else:
            p[0] = p[0] + dot(0, lo, hi)
    pl.semaphore_wait(barrier, len(peers))
    d0 = swap(0)
    rest[0].wait()
    p[1] = dot(1, 0, DEPTH)
    d1 = swap(1)
    settle(0, d0)
    za1u = send(p.at[0, c, a_lo, :], zr1.at[0], up)
    za1d = send(p.at[0, c, a_hi, :], zr1.at[1], down)
    xb0 = xb_send(0)
    rest[1].wait()
    p[2] = dot(2, 0, DEPTH)
    d2 = swap(2)
    settle(1, d1)
    za2u = send(p.at[1, c, a_hi, :], zr2.at[0, 1], up)
    xb1 = xb_send(1)
    rest[2].wait()
    p[3] = dot(3, 0, DEPTH)
    d3 = swap(3)
    settle(2, d2)
    za2d = send(p.at[2, c, a_lo, :], zr2.at[1, 0], down)
    xb2 = xb_send(2)
    xb_settle(0, xb0)
    zb1u = send(p.at[0, c, b_lo, ours], zb1.at[0], up)
    zb1d = send(p.at[0, c, b_hi, ours], zb1.at[1], down)
    za1u.wait_recv()
    p[1, c, a_lo, :] = p[1, c, a_lo, :] + zr1[0]
    za3u = send(p.at[1, c, a_lo, :], zr2.at[0, 0], up)
    za1d.wait_recv()
    p[2, c, a_hi, :] = p[2, c, a_hi, :] + zr1[1]
    za3d = send(p.at[2, c, a_hi, :], zr2.at[1, 1], down)
    settle(3, d3)
    xb3 = xb_send(3)
    xb_settle(1, xb1)
    zb2u = send(p.at[1, c, b_hi, ours], zb2.at[0, 1], up)
    xb_settle(2, xb2)
    zb2d = send(p.at[2, c, b_lo, ours], zb2.at[1, 0], down)
    zb1u.wait_recv()
    p[1, c, b_lo, ours] = p[1, c, b_lo, ours] + zb1[0]
    zb3u = send(p.at[1, c, b_lo, ours], zb2.at[0, 0], up)
    zb1d.wait_recv()
    p[2, c, b_hi, ours] = p[2, c, b_hi, ours] + zb1[1]
    zb3d = send(p.at[2, c, b_hi, ours], zb2.at[1, 1], down)
    for rc in (za2u, za3u, za2d, za3d):
        rc.wait_recv()
    p[3, c, pl.ds(0, A), :] = p[3, c, pl.ds(0, A), :] + zr2[0].reshape(A, 256) + zr2[1].reshape(A, 256)
    xas = send(p.at[3, c, pl.ds(0, A), theirs], xa, mate)
    xb_settle(3, xb3)
    for rc in (zb2u, zb3u, zb2d, zb3d):
        rc.wait_recv()
    pf[pl.ds(A, B), :] = p[3, c, pl.ds(A, B), ours] + zb2[0].reshape(B, 128) + zb2[1].reshape(B, 128)
    fb = send(pf.at[pl.ds(A, B), :], pfr.at[pl.ds(A, B), :], partner)
    xas.wait_recv()
    pf[pl.ds(0, A), :] = p[3, c, pl.ds(0, A), ours] + xa[...]
    fa = send(pf.at[pl.ds(0, A), :], pfr.at[pl.ds(0, A), :], partner)

    def split(value, half):
        hi = value.astype(BF16)
        bhl[half, :, pl.ds(0, 128)] = hi
        bhl[half, :, pl.ds(128, 128)] = (value - hi.astype(F32)).astype(BF16)

    split(pf[...], c)
    lload.wait()
    fb.wait_recv()
    fa.wait_recv()
    split(pfr[...], 1 - c)
    both = lax.dot_general(l[...], bhl[...].reshape(ROWS, 256), CONTRACT0, preferred_element_type=F32)
    rp[...] = (both[:, :128] + both[:, 128:]).reshape(8, 64, 128)

    adds = []
    for dx in (0, 2):
        for dy in (0, 1, 3, 2):
            if dx or dy:
                their_row = ((y + dy) % 4) * 2 + (xh + dx // 2) % 2
                adds.append(send(rp.at[their_row], rr.at[len(adds)], dev(dx=dx, dy=dy)))
    total = rp[row]
    for i, rc in enumerate(adds):
        rc.wait_recv()
        total = total + rr[i]

    def lane(qz, qx):
        return pl.ds(pl.multiple_of(qz * 256 + (qx % 2) * 128, 128), 128)

    def wide(qz):
        return pl.ds(pl.multiple_of(qz * 256, 256), 256)

    out[c, y, xh, :, lane(z, x)] = total

    R = [pl.ds(a, n) for a, n in ROTATIONS]

    def set_x(d, g, half=None):
        qx = (x + d) % 4
        ys = pl.ds(0, 4) if half is None else pl.ds(2 * half, 2)
        return out.at[c, ys, qx // 2, R[0], lane((z + g) % 4, qx)]

    def set_y(d, g, half=None):
        hs = pl.ds(0, 2) if half is None else pl.ds(half, 1)
        return out.at[c, (y + d) % 4, hs, R[1], wide((z + g) % 4)]

    def set_z(d, g, half=None):
        hs = pl.ds(0, 2) if half is None else pl.ds(half, 1)
        return out.at[c, (y + g) % 4, hs, R[2], wide((z + d) % 4)]

    sets = (set_x, set_y, set_z)
    along = ("dx", "dy", "dz")
    second = ("dz", "dz", "dy")
    block = lambda rows: out.at[c, y, xh, rows, lane(z, x)]
    same = lambda ref, device: send(ref, ref, device)

    low, high = R[0], pl.ds(24, 40)
    s1 = [[], []]
    for d in (1, 3, 2):
        s1[0].append(same(block(low), dev(dy=d)))
        s1[1].append(same(block(high), dev(dx=d)))
    s2 = [{}, {}, {}]
    s3 = [{}, {}, {}]
    fw = [{}, {}, {}]
    last = []

    def onward(t, g):
        ref = sets[t](0, g)
        s3[t][g, 1] = same(ref, dev(**{along[t]: 1}))
        s3[t][g, 3] = same(ref, dev(**{along[t]: 3}))
        last.append(same(ref, partner))

    for t in range(3):
        if t < 2:
            for rc in s1[t]:
                rc.wait_recv()
        for d in (1, 3, 2):
            s2[t][d] = same(sets[t](0, 0), dev(**{second[t]: d}))
        onward(t, 0)
    for d in (1, 3, 2):
        for t in range(3):
            s2[t][d].wait_recv()
            onward(t, (4 - d) % 4)
    for g in (0, 3, 1, 2):
        for t in range(3):
            s3[t][g, 1].wait_recv()
            fw[t][g, 0] = same(sets[t](3, g, 0), dev(**{along[t]: 1}))
            last.append(same(sets[t](3, g), partner))
            s3[t][g, 3].wait_recv()
            fw[t][g, 1] = same(sets[t](1, g, 1), dev(**{along[t]: 3}))
            last.append(same(sets[t](1, g), partner))
    for g in (0, 3, 1, 2):
        for t in range(3):
            fw[t][g, 0].wait_recv()
            fw[t][g, 1].wait_recv()
            last.append(same(sets[t](2, g), partner))
    for rc in last:
        rc.wait_recv()
    for rc in sent:
        rc.wait_send()


def call(h, v, l):
    dma = pltpu.SemaphoreType.DMA
    vmem = pltpu.VMEM
    return pl.pallas_call(
        kernel,
        out_shape=jax.ShapeDtypeStruct((2, 4, 2, 64, NVEC), F32),
        in_specs=[pl.BlockSpec(memory_space=pl.ANY)] * 3,
        out_specs=pl.BlockSpec(memory_space=pltpu.VMEM),
        scratch_shapes=[
            vmem((DEPTH, ROWS), BF16),
            vmem((4, DEPTH, 256), BF16),
            vmem((ROWS, 512), BF16),
            vmem((4, 2, HALF, 256), F32),
            vmem((4, HALF, 256), F32),
            vmem((2, A2, 256), F32),
            vmem((2, 2, A2, 256), F32),
            vmem((4, B, 128), F32),
            vmem((2, B2, 128), F32),
            vmem((2, 2, B2, 128), F32),
            vmem((A, 128), F32),
            vmem((HALF, 128), F32),
            vmem((HALF, 128), F32),
            vmem((2, HALF, 256), BF16),
            vmem((8, 64, 128), F32),
            vmem((7, 64, 128), F32),
            dma((16,)),
            dma((NMSG,)),
            dma((NMSG,)),
        ],
        compiler_params=pltpu.CompilerParams(
            collective_id=0, has_side_effects=True, vmem_limit_bytes=56 * 1024 * 1024
        ),
        cost_estimate=pl.CostEstimate(flops=2 * ROWS * DEPTH * NVEC, bytes_accessed=23000000, transcendentals=0),
    )(h, v, l)


def body(h_slab, vectors, left_rows):
    return call(h_slab.T, vectors, left_rows).reshape(NVEC, NVEC)


def solution(mesh):
    in_specs = (P("row", "col"), P("col", None), P("row", None))
    return jax.shard_map(body, mesh=mesh, in_specs=in_specs, out_specs=P(), check_vma=False)
```

```python
import functools

import jax
import jax.numpy as jnp
from jax import lax
from jax.experimental import pallas as pl
from jax.experimental.pallas import tpu as pltpu
from jax.sharding import PartitionSpec as P

MESH = pl.DeviceIdType.MESH
F32 = jnp.float32
BF16 = jnp.bfloat16
DEPTH = 6000
ROWS = 512
HALF = 256
NVEC = 1024
CUTS = ((0, 2048), (2048, 4096), (4096, 6000))
ROTATIONS = ((0, 24), (24, 24), (48, 16))
SWAP, GATHER, PAIR, ROWSUM, PLANE, LINE, OTHER, SENDS = 0, 1, 2, 3, 4, 7, 10, 13
COLS, PAIRED, ROWS_IN, PLANE_IN, LINE_IN, OTHER_IN, ARRIVALS = 4, 5, 6, 9, 21, 33, 35
CONTRACT0 = (((0,), (0,)), ((), ()))


def kernel(h_hbm, v_hbm, l_hbm, out, h, v, ht, gx, l, p, dr, zr, pf, pfr, bhl, rp, rr, lsem, ssem, rsem):
    row, col = lax.axis_index("row"), lax.axis_index("col")
    y, xh = row // 2, row % 2
    z, xl, c = col // 4, (col // 2) % 2, col % 2
    x = xh * 2 + xl

    def dev(dx=0, dy=0, dz=0, core=None, px=None):
        nx = (x + dx) % 4 if px is None else px
        ny, nz = (y + dy) % 4, (z + dz) % 4
        nc = c if core is None else core
        return (ny * 2 + nx // 2, nz * 4 + (nx % 2) * 2 + nc)

    partner = dev(core=1 - c)

    zs = [(z + 2) % 4, (z + 1) % 4, (z + 3) % 4, z]
    lanes = [pl.ds(pl.multiple_of(q * 256, 256), 256) for q in zs]
    loads = []

    def load(src, dst):
        cp = pltpu.make_async_copy(src, dst, lsem.at[len(loads)])
        cp.start()
        loads.append(cp)
        return cp

    first = []
    for lo, hi in CUTS:
        k = pl.ds(lo, hi - lo)
        first.append((load(h_hbm.at[k, :], h.at[k, :]), load(v_hbm.at[k, lanes[0]], v.at[0, k, :])))
    rest = [load(v_hbm.at[:, lanes[s]], v.at[s]) for s in (1, 2, 3)]
    lload = load(l_hbm.at[:, pl.ds(pl.multiple_of(c * 512, 512), 512)], l)

    barrier = pltpu.get_barrier_semaphore()
    peers = [partner]
    for d in (1, 2, 3):
        peers += [dev(dx=d), dev(dy=d), dev(dz=d)]
        for e in (1, 2, 3):
            peers += [dev(dx=d, dy=e), dev(dy=d, dz=e), dev(dz=d, dx=e)]
    for peer in peers:
        pl.semaphore_signal(barrier, inc=1, device_id=peer, device_id_type=MESH)

    def send(src, dst, device, out_sem, in_sem):
        pltpu.make_async_remote_copy(
            src_ref=src, dst_ref=dst, send_sem=ssem.at[out_sem], recv_sem=rsem.at[in_sem], device_id=device, device_id_type=MESH
        ).start()

    def wait(sem, ref):
        pltpu.make_async_copy(ref, ref, sem).wait()

    def multiply(s):
        for j in (0, 1):
            p[s, j] = jnp.dot(ht[pl.ds(j * HALF, HALF), :], v[s], preferred_element_type=F32)

    def swap(s):
        send(p.at[s, 1 - c], dr.at[s], partner, SWAP, s)

    def settle(s):
        wait(rsem.at[s], dr.at[s])
        p[s, c] = p[s, c] + dr[s]

    ours = pl.ds(pl.multiple_of(xl * 128, 128), 128)
    theirs = pl.ds(pl.multiple_of(128 - xl * 128, 128), 128)

    def scatter(s):
        dz = (2, 1, 3, 0)[s]
        send(p.at[s, c, :, theirs], zr.at[2 * s], dev(px=xh * 2 + 1 - xl, dz=dz), GATHER, COLS)
        if dz:
            send(p.at[s, c, :, ours], zr.at[2 * s + 1], dev(dz=dz), GATHER, COLS)

    for i, (lo, hi) in enumerate(CUTS):
        first[i][0].wait()
        first[i][1].wait()
        k = pl.ds(lo, hi - lo)
        ht[:, k] = h[k, :].T
        for j in (0, 1):
            q = jnp.dot(ht[pl.ds(j * HALF, HALF), k], v[0, k, :], preferred_element_type=F32)
            p[0, j] = q if i == 0 else p[0, j] + q
    pl.semaphore_wait(barrier, len(peers))
    swap(0)
    rest[0].wait()
    multiply(1)
    swap(1)
    settle(0)
    scatter(0)
    rest[1].wait()
    multiply(2)
    swap(2)
    settle(1)
    scatter(1)
    rest[2].wait()
    multiply(3)
    swap(3)
    settle(2)
    scatter(2)
    settle(3)
    scatter(3)
    wait(rsem.at[COLS], zr)
    mine = p[3, c, :, ours]
    for i in range(7):
        mine = mine + zr[i]
    pf[...] = mine
    send(pf, pfr, partner, PAIR, PAIRED)

    def split(value, half):
        hi = value.astype(BF16)
        bhl[half, :, pl.ds(0, 128)] = hi
        bhl[half, :, pl.ds(128, 128)] = (value - hi.astype(F32)).astype(BF16)

    split(pf[...], c)
    lload.wait()
    wait(rsem.at[PAIRED], pfr)
    split(pfr[...], 1 - c)
    both = lax.dot_general(l[...], bhl[...].reshape(ROWS, 256), CONTRACT0, preferred_element_type=F32)
    rp[...] = (both[:, :128] + both[:, 128:]).reshape(8, 64, 128)

    R = [pl.ds(a, n) for a, n in ROTATIONS]
    for t in range(3):
        i = 0
        for dx in (0, 2):
            for dy in (0, 1, 3, 2):
                if dx or dy:
                    their_row = ((y + dy) % 4) * 2 + (xh + dx // 2) % 2
                    send(rp.at[their_row, R[t]], rr.at[i, R[t]], dev(dx=dx, dy=dy), ROWSUM, ROWS_IN + t)
                    i += 1

    def lane(qz, qx):
        return pl.ds(pl.multiple_of(qz * 256 + (qx % 2) * 128, 128), 128)

    def wide(qz):
        return pl.ds(pl.multiple_of(qz * 256, 256), 256)

    def set_x(d, g):
        return gx.at[c, (x + d) % 4, (y + g) % 4]

    def set_y(d, g):
        return out.at[c, (y + d) % 4, :, R[1], wide((z + g) % 4)]

    def set_z(d, g):
        qx = (x + g) % 4
        return out.at[c, :, qx // 2, R[2], lane((z + d) % 4, qx)]

    sets = (set_x, set_y, set_z)
    order = (("dz", "dy", "dx"), ("dx", "dz", "dy"), ("dy", "dx", "dz"))
    def spread(half):
        for qx in range(4):
            for qy in range(4):
                for qz in range(4):
                    lanes = pl.ds(qz * 256 + (qx % 2) * 128, 128)
                    out[half, qy, qx // 2, R[0], lanes] = gx[half, qx, qy, qz]

    own = [gx.at[c, x, y, z]] + [out.at[c, y, xh, r, lane(z, x)] for r in R[1:]]

    for t, (_, n) in enumerate(ROTATIONS):
        wait(rsem.at[ROWS_IN + t], rr.at[:, R[t]])
        total = rp[row, R[t]]
        for i in range(7):
            total = total + rr[i, R[t]]
        if t == 0:
            gx[c, x, y, z] = total
        else:
            out[c, y, xh, R[t], lane(z, x)] = total
        for b in (0, 1, 3, 2):
            for a in (1, 3, 2, 0):
                if a or b:
                    device = dev(**{order[t][0]: a, order[t][1]: b})
                    send(own[t], own[t], device, PLANE + t, PLANE_IN + 4 * t + (4 - b) % 4)
    groups = (0, 3, 1, 2)
    for g in groups:
        for t, (_, n) in enumerate(ROTATIONS):
            line = sets[t](0, g)
            wait(rsem.at[PLANE_IN + 4 * t + g], zr.at[pl.ds(0, 4 if g else 3), pl.ds(0, n)])
            for d in (1, 3, 2):
                send(line, line, dev(**{order[t][2]: d}), LINE + t, LINE_IN + 4 * t + g)
            send(line, line, partner, OTHER + t, OTHER_IN + min(t, 1))
    for g in groups:
        for t, (_, n) in enumerate(ROTATIONS):
            wait(rsem.at[LINE_IN + 4 * t + g], zr.at[pl.ds(0, 3), pl.ds(0, 4 * n)])
            for d in (1, 3, 2):
                line = sets[t](d, g)
                send(line, line, partner, OTHER + t, OTHER_IN + min(t, 1))
    low = ROTATIONS[0][1]
    spread(c)
    wait(rsem.at[OTHER_IN], gx.at[1 - c])
    spread(1 - c)
    wait(rsem.at[OTHER_IN + 1], out.at[1 - c, :, :, pl.ds(low, 64 - low), :])
    wait(ssem.at[SWAP], dr)
    wait(ssem.at[GATHER], zr)
    wait(ssem.at[PAIR], pf)
    wait(ssem.at[ROWSUM], rr)
    for t, (_, n) in enumerate(ROTATIONS):
        wait(ssem.at[PLANE + t], zr.at[pl.ds(0, 5), pl.ds(0, 3 * n)])
        wait(ssem.at[LINE + t], zr.at[pl.ds(0, 6), pl.ds(0, 8 * n)])
        wait(ssem.at[OTHER + t], out.at[c, :, :, pl.ds(0, n), :])


def call(h, v, l):
    dma = pltpu.SemaphoreType.DMA
    vmem = pltpu.VMEM
    return pl.pallas_call(
        kernel,
        out_shape=pltpu.VMEM((2, 4, 2, 64, NVEC), F32),
        in_specs=[pl.BlockSpec(memory_space=pltpu.HBM)] * 3,
        out_specs=pl.BlockSpec(memory_space=pltpu.VMEM),
        scratch_shapes=[
            vmem((DEPTH, ROWS), BF16),
            vmem((4, DEPTH, 256), BF16),
            vmem((ROWS, DEPTH), BF16),
            vmem((2, 4, 4, 4, ROTATIONS[0][1], 128), F32),
            vmem((ROWS, 512), BF16),
            vmem((4, 2, HALF, 256), F32),
            vmem((4, HALF, 256), F32),
            vmem((7, HALF, 128), F32),
            vmem((HALF, 128), F32),
            vmem((HALF, 128), F32),
            vmem((2, HALF, 256), BF16),
            vmem((8, 64, 128), F32),
            vmem((7, 64, 128), F32),
            dma((10,)),
            dma((SENDS,)),
            dma((ARRIVALS,)),
        ],
        compiler_params=pltpu.CompilerParams(
            collective_id=0, has_side_effects=True, vmem_limit_bytes=46 * 1024 * 1024
        ),
        cost_estimate=pl.CostEstimate(flops=2 * ROWS * DEPTH * NVEC, bytes_accessed=23000000, transcendentals=0),
    )(h, v, l)


def body(h_slab, vectors, left_rows):
    h, v, l = [pltpu.with_memory_space_constraint(a, pltpu.HBM) for a in (h_slab.T, vectors, left_rows)]
    return call(h, v, l).reshape(NVEC, NVEC)


def solution(mesh):
    in_specs = (P("row", "col"), P("col", None), P("row", None))
    return jax.shard_map(body, mesh=mesh, in_specs=in_specs, out_specs=P(), check_vma=False)
```

```python
import functools

import jax
import jax.numpy as jnp
from jax import lax
from jax.experimental import pallas as pl
from jax.experimental.pallas import tpu as pltpu
from jax.sharding import PartitionSpec as P

MESH = pl.DeviceIdType.MESH
F32 = jnp.float32
BF16 = jnp.bfloat16
DEPTH = 6000
ROWS = 512
HALF = 256
NVEC = 1024
CUTS = ((0, 2048), (2048, 4096), (4096, 6000))
ROTATIONS = ((0, 24), (24, 24), (48, 16))
SWAP, GATHER, PAIR, ROWSUM, PLANE, LINE, OTHER, SENDS = 0, 1, 2, 3, 4, 7, 10, 13
COLS, PAIRED, ROWS_IN, PLANE_IN, LINE_IN, OTHER_IN, PASSED, ARRIVALS = 8, 9, 10, 13, 25, 37, 39, 41
UNITS = ((0, 0), (0, 1), (1, 0), (2, 0), (1, 1), (2, 1), (3, 0), (3, 1))
SETTLE = ((), (0,), (1,), (), (2,), (3,), (4,), (5, 6, 7))
CONTRACT0 = (((0,), (0,)), ((), ()))


def kernel(h_hbm, v_hbm, l_hbm, out, h, v, gx, l, p, dr, zr, zf, pf, pfr, bhl, rp, rr, lsem, ssem, rsem):
    row, col = lax.axis_index("row"), lax.axis_index("col")
    y, xh = row // 2, row % 2
    z, xl, c = col // 4, (col // 2) % 2, col % 2
    x = xh * 2 + xl

    def dev(dx=0, dy=0, dz=0, core=None, px=None):
        nx = (x + dx) % 4 if px is None else px
        ny, nz = (y + dy) % 4, (z + dz) % 4
        nc = c if core is None else core
        return (ny * 2 + nx // 2, nz * 4 + (nx % 2) * 2 + nc)

    partner = dev(core=1 - c)

    zs = [(z + 2) % 4, (z + 1) % 4, (z + 3) % 4, z]
    lanes = [pl.ds(pl.multiple_of(q * 256, 256), 256) for q in zs]
    loads = []

    def load(src, dst):
        cp = pltpu.make_async_copy(src, dst, lsem.at[len(loads)])
        cp.start()
        loads.append(cp)
        return cp

    ours = pl.ds(pl.multiple_of(xl * 128, 128), 128)
    theirs = pl.ds(pl.multiple_of(128 - xl * 128, 128), 128)
    mine_k = pl.ds(pl.multiple_of(c * HALF, HALF), HALF)
    other_k = pl.ds(pl.multiple_of(HALF - c * HALF, HALF), HALF)

    def columns(s, which):
        start = zs[s] * 256 + (xl if which else 1 - xl) * 128
        return pl.ds(pl.multiple_of(start, 128), 128)

    first = []
    for lo, hi in CUTS:
        k = pl.ds(lo, hi - lo)
        first.append((load(h_hbm.at[k, :], h.at[k, :]), load(v_hbm.at[k, columns(0, 0)], v.at[0, k, theirs])))
    later = load(v_hbm.at[:, columns(0, 1)], v.at[0, :, ours])
    rest = [load(v_hbm.at[:, lanes[s]], v.at[s]) for s in (1, 2, 3)]
    lload = load(l_hbm.at[:, pl.ds(pl.multiple_of(c * 512, 512), 512)], l)

    barrier = pltpu.get_barrier_semaphore()
    peers = [partner]
    for d in (1, 2, 3):
        peers += [dev(dx=d), dev(dy=d), dev(dz=d)]
        for e in (1, 2, 3):
            peers += [dev(dx=d, dy=e), dev(dy=d, dz=e), dev(dz=d, dx=e)]
    for peer in peers:
        pl.semaphore_signal(barrier, inc=1, device_id=peer, device_id_type=MESH)

    def send(src, dst, device, out_sem, in_sem):
        pltpu.make_async_remote_copy(
            src_ref=src, dst_ref=dst, send_sem=ssem.at[out_sem], recv_sem=rsem.at[in_sem], device_id=device, device_id_type=MESH
        ).start()

    def wait(sem, ref):
        pltpu.make_async_copy(ref, ref, sem).wait()

    def multiply(u, s, which):
        mine = ours if which else theirs
        if u:
            p[u] = lax.dot_general(v[s, :, mine], h[...], CONTRACT0, preferred_element_type=F32)
            return
        for i, (lo, hi) in enumerate(CUTS):
            for cp in first[i]:
                cp.wait()
            k = pl.ds(lo, hi - lo)
            q = lax.dot_general(v[s, k, mine], h[k, :], CONTRACT0, preferred_element_type=F32)
            p[u] = p[u] + q if i else q

    def settle(u):
        wait(rsem.at[u], dr.at[u])
        p[u, :, mine_k] = p[u, :, mine_k] + dr[u]

    up, down = dev(dz=1), dev(dz=3)
    low, high = pl.ds(0, 64), pl.ds(64, 64)

    def owner(u):
        s, which = UNITS[u]
        return dev(px=x if which else xh * 2 + 1 - xl, dz=(2, 1, 3, 0)[s])

    def scatter(u, rows=None):
        s, which = UNITS[u]
        if s == 0:
            send(p.at[u, low, mine_k], zf.at[0, which], up, GATHER, PASSED)
            send(p.at[u, high, mine_k], zf.at[1, which], down, GATHER, PASSED + 1)
        elif s == 3:
            if which == 0:
                send(p.at[u, :, mine_k], zr.at[4], owner(u), GATHER, COLS)
        else:
            rows = rows or (None, high, low)[s]
            send(p.at[u, rows, mine_k], zr.at[2 * s - 2 + which, rows], owner(u), GATHER, COLS)

    loaded = set()
    for u, (s, which) in enumerate(UNITS):
        if u == 1:
            later.wait()
        if s and s not in loaded:
            rest[s - 1].wait()
            loaded.add(s)
        multiply(u, s, which)
        if u == 0:
            pl.semaphore_wait(barrier, len(peers))
        send(p.at[u, :, other_k], dr.at[u], partner, SWAP, u)
        for w in SETTLE[u]:
            settle(w)
            scatter(w)
    for i, rows in enumerate((low, high)):
        wait(rsem.at[PASSED + i], zf.at[i])
        for u, (s, which) in enumerate(UNITS):
            if s == i + 1:
                p[u, rows, mine_k] = p[u, rows, mine_k] + zf[i, which]
                scatter(u, rows)
    wait(rsem.at[COLS], zr)
    mine = p[7, :, mine_k]
    for i in range(5):
        mine = mine + zr[i]
    pf[...] = mine
    send(pf, pfr, partner, PAIR, PAIRED)

    def split(value, k):
        hi = value.astype(BF16)
        bhl[pl.ds(0, 128), k] = hi
        bhl[pl.ds(128, 128), k] = (value - hi.astype(F32)).astype(BF16)

    split(pf[...], mine_k)
    lload.wait()
    wait(rsem.at[PAIRED], pfr)
    split(pfr[...], other_k)
    both = lax.dot_general(l[...], bhl[...], (((0,), (1,)), ((), ())), preferred_element_type=F32)
    rp[...] = (both[:, :128] + both[:, 128:]).reshape(8, 64, 128)

    R = [pl.ds(a, n) for a, n in ROTATIONS]
    for t in range(3):
        i = 0
        for dx in (0, 2):
            for dy in (0, 1, 3, 2):
                if dx or dy:
                    their_row = ((y + dy) % 4) * 2 + (xh + dx // 2) % 2
                    send(rp.at[their_row, R[t]], rr.at[i, R[t]], dev(dx=dx, dy=dy), ROWSUM, ROWS_IN + t)
                    i += 1

    def lane(qz, qx):
        return pl.ds(pl.multiple_of(qz * 256 + (qx % 2) * 128, 128), 128)

    def wide(qz):
        return pl.ds(pl.multiple_of(qz * 256, 256), 256)

    def set_x(d, g):
        return gx.at[c, (x + d) % 4, (y + g) % 4]

    def set_y(d, g):
        return out.at[c, (y + d) % 4, :, R[1], wide((z + g) % 4)]

    def set_z(d, g):
        qx = (x + g) % 4
        return out.at[c, :, qx // 2, R[2], lane((z + d) % 4, qx)]

    sets = (set_x, set_y, set_z)
    order = (("dz", "dy", "dx"), ("dx", "dz", "dy"), ("dy", "dx", "dz"))
    def spread(half):
        for qx in range(4):
            for qy in range(4):
                for qz in range(4):
                    lanes = pl.ds(qz * 256 + (qx % 2) * 128, 128)
                    out[half, qy, qx // 2, R[0], lanes] = gx[half, qx, qy, qz]

    own = [gx.at[c, x, y, z]] + [out.at[c, y, xh, r, lane(z, x)] for r in R[1:]]

    for t, (_, n) in enumerate(ROTATIONS):
        wait(rsem.at[ROWS_IN + t], rr.at[:, R[t]])
        total = rp[row, R[t]]
        for i in range(7):
            total = total + rr[i, R[t]]
        if t == 0:
            gx[c, x, y, z] = total
        else:
            out[c, y, xh, R[t], lane(z, x)] = total
        for b in (0, 1, 3, 2):
            for a in (1, 3, 2, 0):
                if a or b:
                    device = dev(**{order[t][0]: a, order[t][1]: b})
                    send(own[t], own[t], device, PLANE + t, PLANE_IN + 4 * t + (4 - b) % 4)
    groups = (0, 3, 1, 2)
    for g in groups:
        for t, (_, n) in enumerate(ROTATIONS):
            line = sets[t](0, g)
            wait(rsem.at[PLANE_IN + 4 * t + g], dr.at[pl.ds(0, 4 if g else 3), pl.ds(0, n), pl.ds(0, 128)])
            for d in (1, 3, 2):
                send(line, line, dev(**{order[t][2]: d}), LINE + t, LINE_IN + 4 * t + g)
            send(line, line, partner, OTHER + t, OTHER_IN + min(t, 1))
    for g in groups:
        for t, (_, n) in enumerate(ROTATIONS):
            wait(rsem.at[LINE_IN + 4 * t + g], dr.at[pl.ds(0, 3), pl.ds(0, 2 * n)])
            for d in (1, 3, 2):
                line = sets[t](d, g)
                send(line, line, partner, OTHER + t, OTHER_IN + min(t, 1))
    low = ROTATIONS[0][1]
    spread(c)
    wait(rsem.at[OTHER_IN], gx.at[1 - c])
    spread(1 - c)
    wait(rsem.at[OTHER_IN + 1], out.at[1 - c, :, :, pl.ds(low, 64 - low), :])
    wait(ssem.at[SWAP], dr)
    wait(ssem.at[GATHER], dr.at[pl.ds(0, 7)])
    wait(ssem.at[PAIR], pf)
    wait(ssem.at[ROWSUM], rr)
    for t, (_, n) in enumerate(ROTATIONS):
        wait(ssem.at[PLANE + t], dr.at[pl.ds(0, 5), pl.ds(0, 3 * n), pl.ds(0, 128)])
        wait(ssem.at[LINE + t], dr.at[pl.ds(0, 6), pl.ds(0, 4 * n)])
        wait(ssem.at[OTHER + t], out.at[c, :, :, pl.ds(0, n), :])


def call(h, v, l):
    dma = pltpu.SemaphoreType.DMA
    vmem = pltpu.VMEM
    return pl.pallas_call(
        kernel,
        out_shape=pltpu.VMEM((2, 4, 2, 64, NVEC), F32),
        in_specs=[pl.BlockSpec(memory_space=pltpu.HBM)] * 3,
        out_specs=pl.BlockSpec(memory_space=pltpu.VMEM),
        scratch_shapes=[
            vmem((DEPTH, ROWS), BF16),
            vmem((4, DEPTH, 256), BF16),
            vmem((2, 4, 4, 4, ROTATIONS[0][1], 128), F32),
            vmem((ROWS, 512), BF16),
            vmem((8, 128, ROWS), F32),
            vmem((8, 128, HALF), F32),
            vmem((5, 128, HALF), F32),
            vmem((2, 2, 64, HALF), F32),
            vmem((128, HALF), F32),
            vmem((128, HALF), F32),
            vmem((2 * 128, ROWS), BF16),
            vmem((8, 64, 128), F32),
            vmem((7, 64, 128), F32),
            dma((11,)),
            dma((SENDS,)),
            dma((ARRIVALS,)),
        ],
        compiler_params=pltpu.CompilerParams(
            collective_id=0, has_side_effects=True, vmem_limit_bytes=46 * 1024 * 1024
        ),
        cost_estimate=pl.CostEstimate(flops=2 * ROWS * DEPTH * NVEC, bytes_accessed=23000000, transcendentals=0),
    )(h, v, l)


def body(h_slab, vectors, left_rows):
    h, v, l = [pltpu.with_memory_space_constraint(a, pltpu.HBM) for a in (h_slab.T, vectors, left_rows)]
    return call(h, v, l).reshape(NVEC, NVEC)


def solution(mesh):
    in_specs = (P("row", "col"), P("col", None), P("row", None))
    return jax.shard_map(body, mesh=mesh, in_specs=in_specs, out_specs=P(), check_vma=False)
```

```python
import functools

import jax
import jax.numpy as jnp
from jax import lax
from jax.experimental import pallas as pl
from jax.experimental.pallas import tpu as pltpu
from jax.sharding import PartitionSpec as P

MESH = pl.DeviceIdType.MESH
F32 = jnp.float32
BF16 = jnp.bfloat16
DEPTH = 6000
ROWS = 512
HALF = 256
NVEC = 1024
CUTS = ((0, 2048), (2048, 4096), (4096, 6000))
ROTATIONS = ((0, 24), (24, 24), (48, 16))
SWAP, GATHER, PAIR, ROWSUM, PLANE, LINE, OTHER, SENDS = 0, 1, 2, 3, 4, 7, 10, 13
COLS, PAIRED, ROWS_IN, PLANE_IN, LINE_IN, OTHER_IN, PASSED, ARRIVALS = 8, 9, 10, 13, 25, 37, 39, 41
UNITS = ((3, 0), (0, 0), (0, 1), (1, 0), (2, 0), (1, 1), (2, 1), (3, 1))
SETTLE = ((), (0,), (1,), (2,), (3,), (4,), (5,), (6,))
CONTRACT0 = (((0,), (0,)), ((), ()))


def kernel(h_hbm, v_hbm, l_hbm, out, h, v, gx, l, p, dr, zr, zf, pf, pfr, bhl, rp, rr, lsem, ssem, rsem):
    row, col = lax.axis_index("row"), lax.axis_index("col")
    y, xh = row // 2, row % 2
    z, xl, c = col // 4, (col // 2) % 2, col % 2
    x = xh * 2 + xl

    def dev(dx=0, dy=0, dz=0, core=None, px=None):
        nx = (x + dx) % 4 if px is None else px
        ny, nz = (y + dy) % 4, (z + dz) % 4
        nc = c if core is None else core
        return (ny * 2 + nx // 2, nz * 4 + (nx % 2) * 2 + nc)

    partner = dev(core=1 - c)

    zs = [(z + 2) % 4, (z + 1) % 4, (z + 3) % 4, z]
    lanes = [pl.ds(pl.multiple_of(q * 256, 256), 256) for q in zs]
    loads = []

    def load(src, dst):
        cp = pltpu.make_async_copy(src, dst, lsem.at[len(loads)])
        cp.start()
        loads.append(cp)
        return cp

    ours = pl.ds(pl.multiple_of(xl * 128, 128), 128)
    theirs = pl.ds(pl.multiple_of(128 - xl * 128, 128), 128)
    mine_k = pl.ds(pl.multiple_of(c * HALF, HALF), HALF)
    other_k = pl.ds(pl.multiple_of(HALF - c * HALF, HALF), HALF)

    def columns(s, which):
        start = zs[s] * 256 + (xl if which else 1 - xl) * 128
        return pl.ds(pl.multiple_of(start, 128), 128)

    first = []
    for lo, hi in CUTS:
        k = pl.ds(lo, hi - lo)
        first.append((load(h_hbm.at[k, :], h.at[k, :]), load(v_hbm.at[k, columns(3, 0)], v.at[3, k, theirs])))
    rest = [load(v_hbm.at[:, lanes[s]], v.at[s]) for s in (0, 1, 2)]
    rest.append(load(v_hbm.at[:, columns(3, 1)], v.at[3, :, ours]))
    lload = load(l_hbm.at[:, pl.ds(pl.multiple_of(c * 512, 512), 512)], l)

    barrier = pltpu.get_barrier_semaphore()
    peers = [partner]
    for d in (1, 2, 3):
        peers += [dev(dx=d), dev(dy=d), dev(dz=d)]
        for e in (1, 2, 3):
            peers += [dev(dx=d, dy=e), dev(dy=d, dz=e), dev(dz=d, dx=e)]
    for peer in peers:
        pl.semaphore_signal(barrier, inc=1, device_id=peer, device_id_type=MESH)

    def send(src, dst, device, out_sem, in_sem):
        pltpu.make_async_remote_copy(
            src_ref=src, dst_ref=dst, send_sem=ssem.at[out_sem], recv_sem=rsem.at[in_sem], device_id=device, device_id_type=MESH
        ).start()

    def wait(sem, ref):
        pltpu.make_async_copy(ref, ref, sem).wait()

    def multiply(u, s, which):
        mine = ours if which else theirs
        if u:
            p[u] = lax.dot_general(v[s, :, mine], h[...], CONTRACT0, preferred_element_type=F32)
            return
        for i, (lo, hi) in enumerate(CUTS):
            for cp in first[i]:
                cp.wait()
            k = pl.ds(lo, hi - lo)
            q = lax.dot_general(v[s, k, mine], h[k, :], CONTRACT0, preferred_element_type=F32)
            p[u] = p[u] + q if i else q

    def settle(u):
        wait(rsem.at[u], dr.at[u])
        p[u, :, mine_k] = p[u, :, mine_k] + dr[u]

    up, down = dev(dz=1), dev(dz=3)
    low, high = pl.ds(0, 64), pl.ds(64, 64)

    def owner(u):
        s, which = UNITS[u]
        return dev(px=x if which else xh * 2 + 1 - xl, dz=(2, 1, 3, 0)[s])

    def scatter(u, rows=None):
        s, which = UNITS[u]
        if s == 0:
            send(p.at[u, low, mine_k], zf.at[0, which], up, GATHER, PASSED)
            send(p.at[u, high, mine_k], zf.at[1, which], down, GATHER, PASSED + 1)
        elif s == 3:
            if which == 0:
                send(p.at[u, :, mine_k], zr.at[4], owner(u), GATHER, COLS)
        else:
            rows = rows or (None, high, low)[s]
            send(p.at[u, rows, mine_k], zr.at[2 * s - 2 + which, rows], owner(u), GATHER, COLS)

    loaded = set()
    for u, (s, which) in enumerate(UNITS):
        if u and s not in loaded:
            rest[s].wait()
            loaded.add(s)
        multiply(u, s, which)
        if u == 0:
            pl.semaphore_wait(barrier, len(peers))
        send(p.at[u, :, other_k], dr.at[u], partner, SWAP, u)
        for w in SETTLE[u]:
            settle(w)
            scatter(w)
    for i, rows in enumerate((low, high)):
        wait(rsem.at[PASSED + i], zf.at[i])
        for u, (s, which) in enumerate(UNITS):
            if s == i + 1:
                p[u, rows, mine_k] = p[u, rows, mine_k] + zf[i, which]
                scatter(u, rows)
    settle(7)
    wait(rsem.at[COLS], zr)
    mine = p[7, :, mine_k]
    for i in range(5):
        mine = mine + zr[i]
    pf[...] = mine
    send(pf, pfr, partner, PAIR, PAIRED)

    def split(value, k):
        hi = value.astype(BF16)
        bhl[pl.ds(0, 128), k] = hi
        bhl[pl.ds(128, 128), k] = (value - hi.astype(F32)).astype(BF16)

    split(pf[...], mine_k)
    lload.wait()
    wait(rsem.at[PAIRED], pfr)
    split(pfr[...], other_k)
    both = lax.dot_general(l[...], bhl[...], (((0,), (1,)), ((), ())), preferred_element_type=F32)
    rp[...] = (both[:, :128] + both[:, 128:]).reshape(8, 64, 128)

    R = [pl.ds(a, n) for a, n in ROTATIONS]
    for t in range(3):
        i = 0
        for dx in (0, 2):
            for dy in (0, 1, 3, 2):
                if dx or dy:
                    their_row = ((y + dy) % 4) * 2 + (xh + dx // 2) % 2
                    send(rp.at[their_row, R[t]], rr.at[i, R[t]], dev(dx=dx, dy=dy), ROWSUM, ROWS_IN + t)
                    i += 1

    def lane(qz, qx):
        return pl.ds(pl.multiple_of(qz * 256 + (qx % 2) * 128, 128), 128)

    def wide(qz):
        return pl.ds(pl.multiple_of(qz * 256, 256), 256)

    def set_x(d, g):
        return gx.at[c, (x + d) % 4, (y + g) % 4]

    def set_y(d, g):
        return out.at[c, (y + d) % 4, :, R[1], wide((z + g) % 4)]

    def set_z(d, g):
        qx = (x + g) % 4
        return out.at[c, :, qx // 2, R[2], lane((z + d) % 4, qx)]

    sets = (set_x, set_y, set_z)
    order = (("dz", "dy", "dx"), ("dx", "dz", "dy"), ("dy", "dx", "dz"))
    def spread(half):
        for qx in range(4):
            for qy in range(4):
                for qz in range(4):
                    lanes = pl.ds(qz * 256 + (qx % 2) * 128, 128)
                    out[half, qy, qx // 2, R[0], lanes] = gx[half, qx, qy, qz]

    own = [gx.at[c, x, y, z]] + [out.at[c, y, xh, r, lane(z, x)] for r in R[1:]]

    for t, (_, n) in enumerate(ROTATIONS):
        wait(rsem.at[ROWS_IN + t], rr.at[:, R[t]])
        total = rp[row, R[t]]
        for i in range(7):
            total = total + rr[i, R[t]]
        if t == 0:
            gx[c, x, y, z] = total
        else:
            out[c, y, xh, R[t], lane(z, x)] = total
        for b in (0, 1, 3, 2):
            for a in (1, 3, 2, 0):
                if a or b:
                    device = dev(**{order[t][0]: a, order[t][1]: b})
                    send(own[t], own[t], device, PLANE + t, PLANE_IN + 4 * t + (4 - b) % 4)
    groups = (0, 3, 1, 2)
    for g in groups:
        for t, (_, n) in enumerate(ROTATIONS):
            line = sets[t](0, g)
            wait(rsem.at[PLANE_IN + 4 * t + g], dr.at[pl.ds(0, 4 if g else 3), pl.ds(0, n), pl.ds(0, 128)])
            for d in (1, 3, 2):
                send(line, line, dev(**{order[t][2]: d}), LINE + t, LINE_IN + 4 * t + g)
            send(line, line, partner, OTHER + t, OTHER_IN + min(t, 1))
    for g in groups:
        for t, (_, n) in enumerate(ROTATIONS):
            wait(rsem.at[LINE_IN + 4 * t + g], dr.at[pl.ds(0, 3), pl.ds(0, 2 * n)])
            for d in (1, 3, 2):
                line = sets[t](d, g)
                send(line, line, partner, OTHER + t, OTHER_IN + min(t, 1))
    low = ROTATIONS[0][1]
    spread(c)
    wait(rsem.at[OTHER_IN], gx.at[1 - c])
    spread(1 - c)
    wait(rsem.at[OTHER_IN + 1], out.at[1 - c, :, :, pl.ds(low, 64 - low), :])
    wait(ssem.at[SWAP], dr)
    wait(ssem.at[GATHER], dr.at[pl.ds(0, 7)])
    wait(ssem.at[PAIR], pf)
    wait(ssem.at[ROWSUM], rr)
    for t, (_, n) in enumerate(ROTATIONS):
        wait(ssem.at[PLANE + t], dr.at[pl.ds(0, 5), pl.ds(0, 3 * n), pl.ds(0, 128)])
        wait(ssem.at[LINE + t], dr.at[pl.ds(0, 6), pl.ds(0, 4 * n)])
        wait(ssem.at[OTHER + t], out.at[c, :, :, pl.ds(0, n), :])


def call(h, v, l):
    dma = pltpu.SemaphoreType.DMA
    vmem = pltpu.VMEM
    return pl.pallas_call(
        kernel,
        out_shape=pltpu.VMEM((2, 4, 2, 64, NVEC), F32),
        in_specs=[pl.BlockSpec(memory_space=pltpu.HBM)] * 3,
        out_specs=pl.BlockSpec(memory_space=pltpu.VMEM),
        scratch_shapes=[
            vmem((DEPTH, ROWS), BF16),
            vmem((4, DEPTH, 256), BF16),
            vmem((2, 4, 4, 4, ROTATIONS[0][1], 128), F32),
            vmem((ROWS, 512), BF16),
            vmem((8, 128, ROWS), F32),
            vmem((8, 128, HALF), F32),
            vmem((5, 128, HALF), F32),
            vmem((2, 2, 64, HALF), F32),
            vmem((128, HALF), F32),
            vmem((128, HALF), F32),
            vmem((2 * 128, ROWS), BF16),
            vmem((8, 64, 128), F32),
            vmem((7, 64, 128), F32),
            dma((11,)),
            dma((SENDS,)),
            dma((ARRIVALS,)),
        ],
        compiler_params=pltpu.CompilerParams(
            collective_id=0, has_side_effects=True, vmem_limit_bytes=46 * 1024 * 1024
        ),
        cost_estimate=pl.CostEstimate(flops=2 * ROWS * DEPTH * NVEC, bytes_accessed=23000000, transcendentals=0),
    )(h, v, l)


def body(h_slab, vectors, left_rows):
    h, v, l = [pltpu.with_memory_space_constraint(a, pltpu.HBM) for a in (h_slab.T, vectors, left_rows)]
    return call(h, v, l).reshape(NVEC, NVEC)


def solution(mesh):
    in_specs = (P("row", "col"), P("col", None), P("row", None))
    return jax.shard_map(body, mesh=mesh, in_specs=in_specs, out_specs=P(), check_vma=False)
```

```python
import functools

import jax
import jax.numpy as jnp
from jax import lax
from jax.experimental import pallas as pl
from jax.experimental.pallas import tpu as pltpu
from jax.sharding import PartitionSpec as P

MESH = pl.DeviceIdType.MESH
F32 = jnp.float32
BF16 = jnp.bfloat16
DEPTH = 6000
ROWS = 512
HALF = 256
NVEC = 1024
CUTS = ((0, 2048), (2048, 4096), (4096, 6000))
ROTATIONS = ((0, 24), (24, 24), (48, 16))
SWAP, GATHER, PAIR, ROWSUM, PLANE, LINE, OTHER, SENDS = 0, 1, 2, 3, 4, 7, 10, 13
COLS, PAIRED, ROWS_IN, PLANE_IN, LINE_IN, OTHER_IN, PASSED, ARRIVALS = 8, 9, 10, 13, 25, 37, 39, 41
UNITS = ((3, 0), (0, 0), (0, 1), (1, 0), (2, 0), (1, 1), (2, 1), (3, 1))
SETTLE = ((), (0,), (1,), (2,), (3,), (4,), (5,), (6,))
CONTRACT0 = (((0,), (0,)), ((), ()))


def kernel(h_hbm, v_hbm, l_hbm, out, h, v, gx, l, p, dr, zr, zf, pf, pfr, bhl, rp, rr, lsem, ssem, rsem):
    row, col = lax.axis_index("row"), lax.axis_index("col")
    y, xh = row // 2, row % 2
    z, xl, c = col // 4, (col // 2) % 2, col % 2
    x = xh * 2 + xl

    def dev(dx=0, dy=0, dz=0, core=None, px=None):
        nx = (x + dx) % 4 if px is None else px
        ny, nz = (y + dy) % 4, (z + dz) % 4
        nc = c if core is None else core
        return (ny * 2 + nx // 2, nz * 4 + (nx % 2) * 2 + nc)

    partner = dev(core=1 - c)

    zs = [(z + 2) % 4, (z + 1) % 4, (z + 3) % 4, z]
    lanes = [pl.ds(pl.multiple_of(q * 256, 256), 256) for q in zs]
    loads = []

    def load(src, dst):
        cp = pltpu.make_async_copy(src, dst, lsem.at[len(loads)])
        cp.start()
        loads.append(cp)
        return cp

    ours = pl.ds(pl.multiple_of(xl * 128, 128), 128)
    theirs = pl.ds(pl.multiple_of(128 - xl * 128, 128), 128)
    mine_k = pl.ds(pl.multiple_of(c * HALF, HALF), HALF)
    other_k = pl.ds(pl.multiple_of(HALF - c * HALF, HALF), HALF)

    def columns(s, which):
        start = zs[s] * 256 + (xl if which else 1 - xl) * 128
        return pl.ds(pl.multiple_of(start, 128), 128)

    first = []
    for lo, hi in CUTS:
        k = pl.ds(lo, hi - lo)
        first.append((load(h_hbm.at[k, :], h.at[k, :]), load(v_hbm.at[k, columns(3, 0)], v.at[3, k, theirs])))
    rest = [load(v_hbm.at[:, lanes[s]], v.at[s]) for s in (0, 1, 2)]
    rest.append(load(v_hbm.at[:, columns(3, 1)], v.at[3, :, ours]))
    lload = load(l_hbm.at[:, pl.ds(pl.multiple_of(c * 512, 512), 512)], l)

    barrier = pltpu.get_barrier_semaphore()
    peers = [partner]
    for d in (1, 2, 3):
        peers += [dev(dx=d), dev(dy=d), dev(dz=d)]
        for e in (1, 2, 3):
            peers += [dev(dx=d, dy=e), dev(dy=d, dz=e), dev(dz=d, dx=e)]
    for peer in peers:
        pl.semaphore_signal(barrier, inc=1, device_id=peer, device_id_type=MESH)

    def send(src, dst, device, out_sem, in_sem):
        pltpu.make_async_remote_copy(
            src_ref=src, dst_ref=dst, send_sem=ssem.at[out_sem], recv_sem=rsem.at[in_sem], device_id=device, device_id_type=MESH
        ).start()

    def wait(sem, ref):
        pltpu.make_async_copy(ref, ref, sem).wait()

    def multiply(u, s, which):
        mine = ours if which else theirs
        if u:
            p[u] = lax.dot_general(v[s, :, mine], h[...], CONTRACT0, preferred_element_type=F32)
            return
        for i, (lo, hi) in enumerate(CUTS):
            for cp in first[i]:
                cp.wait()
            k = pl.ds(lo, hi - lo)
            q = lax.dot_general(v[s, k, mine], h[k, :], CONTRACT0, preferred_element_type=F32)
            p[u] = p[u] + q if i else q

    def settle(u):
        wait(rsem.at[u], dr.at[u])
        p[u, :, mine_k] = p[u, :, mine_k] + dr[u]

    up, down = dev(dz=1), dev(dz=3)
    low, high = pl.ds(0, 64), pl.ds(64, 64)

    def owner(u):
        s, which = UNITS[u]
        return dev(px=x if which else xh * 2 + 1 - xl, dz=(2, 1, 3, 0)[s])

    def scatter(u, rows=None):
        s, which = UNITS[u]
        if s == 0:
            send(p.at[u, low, mine_k], zf.at[0, which], up, GATHER, PASSED)
            send(p.at[u, high, mine_k], zf.at[1, which], down, GATHER, PASSED + 1)
        elif s == 3:
            if which == 0:
                send(p.at[u, :, mine_k], zr.at[4], owner(u), GATHER, COLS)
        else:
            rows = rows or (None, high, low)[s]
            send(p.at[u, rows, mine_k], zr.at[2 * s - 2 + which, rows], owner(u), GATHER, COLS)

    loaded = set()
    for u, (s, which) in enumerate(UNITS):
        if u and s not in loaded:
            rest[s].wait()
            loaded.add(s)
        multiply(u, s, which)
        if u == 0:
            pl.semaphore_wait(barrier, len(peers))
        send(p.at[u, :, other_k], dr.at[u], partner, SWAP, u)
        for w in SETTLE[u]:
            settle(w)
            scatter(w)
    for i, rows in enumerate((low, high)):
        wait(rsem.at[PASSED + i], zf.at[i])
        for u, (s, which) in enumerate(UNITS):
            if s == i + 1:
                p[u, rows, mine_k] = p[u, rows, mine_k] + zf[i, which]
                scatter(u, rows)
    settle(7)
    wait(rsem.at[COLS], zr)
    mine = p[7, :, mine_k]
    for i in range(5):
        mine = mine + zr[i]
    pf[...] = mine
    send(pf, pfr, partner, PAIR, PAIRED)

    def split(value, k):
        hi = value.astype(BF16)
        bhl[pl.ds(0, 128), k] = hi
        bhl[pl.ds(128, 128), k] = (value - hi.astype(F32)).astype(BF16)

    split(pf[...], mine_k)
    lload.wait()
    wait(rsem.at[PAIRED], pfr)
    split(pfr[...], other_k)
    both = lax.dot_general(l[...], bhl[...], (((0,), (1,)), ((), ())), preferred_element_type=F32)
    rp[...] = (both[:, :128] + both[:, 128:]).reshape(8, 64, 128)

    R = [pl.ds(a, n) for a, n in ROTATIONS]
    for t in range(3):
        i = 0
        for dx in (2, 0):
            for dy in (2, 1, 3, 0):
                if dx or dy:
                    their_row = ((y + dy) % 4) * 2 + (xh + dx // 2) % 2
                    send(rp.at[their_row, R[t]], rr.at[i, R[t]], dev(dx=dx, dy=dy), ROWSUM, ROWS_IN + t)
                    i += 1

    def lane(qz, qx):
        return pl.ds(pl.multiple_of(qz * 256 + (qx % 2) * 128, 128), 128)

    def wide(qz):
        return pl.ds(pl.multiple_of(qz * 256, 256), 256)

    def set_x(d, g):
        return gx.at[c, (x + d) % 4, (y + g) % 4]

    def set_y(d, g):
        return out.at[c, (y + d) % 4, :, R[1], wide((z + g) % 4)]

    def set_z(d, g):
        qx = (x + g) % 4
        return out.at[c, :, qx // 2, R[2], lane((z + d) % 4, qx)]

    sets = (set_x, set_y, set_z)
    order = (("dz", "dy", "dx"), ("dx", "dz", "dy"), ("dy", "dx", "dz"))
    def spread(half):
        for qx in range(4):
            for qy in range(4):
                for qz in range(4):
                    lanes = pl.ds(qz * 256 + (qx % 2) * 128, 128)
                    out[half, qy, qx // 2, R[0], lanes] = gx[half, qx, qy, qz]

    own = [gx.at[c, x, y, z]] + [out.at[c, y, xh, r, lane(z, x)] for r in R[1:]]

    for t, (_, n) in enumerate(ROTATIONS):
        wait(rsem.at[ROWS_IN + t], rr.at[:, R[t]])
        total = rp[row, R[t]]
        for i in range(7):
            total = total + rr[i, R[t]]
        if t == 0:
            gx[c, x, y, z] = total
        else:
            out[c, y, xh, R[t], lane(z, x)] = total
        for b in (0, 1, 3, 2):
            for a in (1, 3, 2, 0):
                if a or b:
                    device = dev(**{order[t][0]: a, order[t][1]: b})
                    send(own[t], own[t], device, PLANE + t, PLANE_IN + 4 * t + (4 - b) % 4)
    groups = (0, 3, 1, 2)
    for g in groups:
        for t, (_, n) in enumerate(ROTATIONS):
            line = sets[t](0, g)
            wait(rsem.at[PLANE_IN + 4 * t + g], dr.at[pl.ds(0, 4 if g else 3), pl.ds(0, n), pl.ds(0, 128)])
            for d in (1, 3, 2):
                send(line, line, dev(**{order[t][2]: d}), LINE + t, LINE_IN + 4 * t + g)
            send(line, line, partner, OTHER + t, OTHER_IN + min(t, 1))
    for g in groups:
        for t, (_, n) in enumerate(ROTATIONS):
            wait(rsem.at[LINE_IN + 4 * t + g], dr.at[pl.ds(0, 3), pl.ds(0, 2 * n)])
            for d in (1, 3, 2):
                line = sets[t](d, g)
                send(line, line, partner, OTHER + t, OTHER_IN + min(t, 1))
    low = ROTATIONS[0][1]
    spread(c)
    wait(rsem.at[OTHER_IN], gx.at[1 - c])
    spread(1 - c)
    wait(rsem.at[OTHER_IN + 1], out.at[1 - c, :, :, pl.ds(low, 64 - low), :])
    wait(ssem.at[SWAP], dr)
    wait(ssem.at[GATHER], dr.at[pl.ds(0, 7)])
    wait(ssem.at[PAIR], pf)
    wait(ssem.at[ROWSUM], rr)
    for t, (_, n) in enumerate(ROTATIONS):
        wait(ssem.at[PLANE + t], dr.at[pl.ds(0, 5), pl.ds(0, 3 * n), pl.ds(0, 128)])
        wait(ssem.at[LINE + t], dr.at[pl.ds(0, 6), pl.ds(0, 4 * n)])
        wait(ssem.at[OTHER + t], out.at[c, :, :, pl.ds(0, n), :])


def call(h, v, l):
    dma = pltpu.SemaphoreType.DMA
    vmem = pltpu.VMEM
    return pl.pallas_call(
        kernel,
        out_shape=pltpu.VMEM((2, 4, 2, 64, NVEC), F32),
        in_specs=[pl.BlockSpec(memory_space=pltpu.HBM)] * 3,
        out_specs=pl.BlockSpec(memory_space=pltpu.VMEM),
        scratch_shapes=[
            vmem((DEPTH, ROWS), BF16),
            vmem((4, DEPTH, 256), BF16),
            vmem((2, 4, 4, 4, ROTATIONS[0][1], 128), F32),
            vmem((ROWS, 512), BF16),
            vmem((8, 128, ROWS), F32),
            vmem((8, 128, HALF), F32),
            vmem((5, 128, HALF), F32),
            vmem((2, 2, 64, HALF), F32),
            vmem((128, HALF), F32),
            vmem((128, HALF), F32),
            vmem((2 * 128, ROWS), BF16),
            vmem((8, 64, 128), F32),
            vmem((7, 64, 128), F32),
            dma((11,)),
            dma((SENDS,)),
            dma((ARRIVALS,)),
        ],
        compiler_params=pltpu.CompilerParams(
            collective_id=0, has_side_effects=True, vmem_limit_bytes=46 * 1024 * 1024
        ),
        cost_estimate=pl.CostEstimate(flops=2 * ROWS * DEPTH * NVEC, bytes_accessed=23000000, transcendentals=0),
    )(h, v, l)


def body(h_slab, vectors, left_rows):
    h, v, l = [pltpu.with_memory_space_constraint(a, pltpu.HBM) for a in (h_slab.T, vectors, left_rows)]
    return call(h, v, l).reshape(NVEC, NVEC)


def solution(mesh):
    in_specs = (P("row", "col"), P("col", None), P("row", None))
    return jax.shard_map(body, mesh=mesh, in_specs=in_specs, out_specs=P(), check_vma=False)
```
